1024 devices in a mesh: dp: 2 (over y_hi), ctx: 128 (over z, x), tp: 4 (over y_lo, core).
Axes of the slice: x: 4, y: 4 (y_hi: 2, y_lo: 2; y = y_hi * 2 + y_lo), z: 32, core: 2. Of those that a mesh axis runs over, the one named last changes fastest.
Arguments:
- queries: bfloat16 [4, 16384, 4096], P('dp', 'ctx', 'tp'), may hold values from -6 to 6
- keys: bfloat16 [4, 16384, 512], P('dp', 'ctx', 'tp'), may hold values from -6 to 6
- values: bfloat16 [4, 16384, 512], P('dp', 'ctx', 'tp'), may hold values from -6 to 6
- output_gradient: bfloat16 [4, 16384, 4096], P('dp', 'ctx', 'tp'), may hold values from -6 to 6
- sinks: float32 [64], P('tp'), may hold values from -1 to 3
- doc_starts: int32 [4, 64], P('dp'), may hold values from 0 to 32768, as said below
- valid_counts: int32 [4, 128], P('dp'), may hold values from 64 to 128
Outputs:
- query_grad: bfloat16 [4, 16384, 4096], P('dp', 'ctx', 'tp')
- key_grad: bfloat16 [4, 16384, 512], P('dp', 'ctx', 'tp')
- value_grad: bfloat16 [4, 16384, 512], P('dp', 'ctx', 'tp')
- sink_grad: float32 [64], P('tp')
The draws below stay inside these ranges and needn't reach their ends.
Inputs may be any that keep to these rules, and one draw needn't show every extreme that they name: `doc_starts`: each row is strictly increasing, begins with 0 and ends with 32768; a start at or past 16384 opens no document.
All inputs are finite; a program needn't handle non-finite values.
Results may differ from the reference program's by a relative error of at most 0.0093.
Values may be sent and summed in bfloat16 or wider, within the bound.
A program may use at most 64 MiB of HBM per device.

```python
import jax
import jax.numpy as jnp
from jax import lax

QUERY_HEADS = 64
KEY_VALUE_HEADS = 8
HEAD_DIMENSION = 64
WINDOW_LENGTH = 128
CTX_TOK = 128
DOCS = 64
SEQUENCE_LENGTH = 16384
BATCH_SEQUENCES = 4
N_CTX = 128


def draw_queries(key, part):
    regular_portion = jax.random.normal(jax.random.fold_in(key, 1), (BATCH_SEQUENCES, SEQUENCE_LENGTH, QUERY_HEADS * HEAD_DIMENSION), jnp.float32)
    result = jnp.clip(regular_portion, -6.0, 6.0)
    return result.astype(jnp.bfloat16)


def draw_keys(key, part):
    regular_portion = jax.random.normal(jax.random.fold_in(key, 2), (BATCH_SEQUENCES, SEQUENCE_LENGTH, KEY_VALUE_HEADS * HEAD_DIMENSION), jnp.float32)
    result = jnp.clip(regular_portion, -6.0, 6.0)
    return result.astype(jnp.bfloat16)


def draw_doc_starts(key, part):
    spacing = jax.random.randint(jax.random.fold_in(key, 3), (BATCH_SEQUENCES, DOCS), 1, 2 * SEQUENCE_LENGTH // DOCS)
    running = jnp.cumsum(spacing, axis=1)
    starts = (running - spacing[:, :1]).astype(jnp.int32)
    last_column = jnp.arange(DOCS, dtype=jnp.int32)[None, :] == DOCS - 1
    return jnp.where(last_column, jnp.int32(2 * SEQUENCE_LENGTH), starts).astype(jnp.int32)


def place_ends(values, stream_key, least, top_value):
    longest = values.shape.index(max(values.shape))
    spots = []
    for shift in (0, 1):
        where = [jax.random.randint(jax.random.fold_in(stream_key, axis), (), 0, length) for axis, length in enumerate(values.shape)]
        where[longest] = (where[longest] + shift) % values.shape[longest]
        spots.append(tuple(where))
    return values.at[spots[0]].set(least).at[spots[1]].set(top_value)


def level_of(own_key, extent, cuts, low, top_value):
    loudness, own = 1.0, jax.random.fold_in(own_key, 6)
    for dim, shards_of in cuts:
        heights = jnp.exp(jax.random.uniform(jax.random.fold_in(own, dim), (shards_of,), jnp.float32, low / len(cuts), top_value / len(cuts)))
        loudness = loudness * jnp.repeat(heights, extent[dim] // shards_of).reshape([-1 if axis == dim else 1 for axis in range(len(extent))])
    return loudness


def normal_values(rng, dims, width, reach, shards=(), held_as=jnp.bfloat16):
    drawn = jax.random.normal(rng, dims, jnp.float32) * width
    if len(shards) > 0:
        drawn = level_of(rng, dims, shards, -0.22, 0.18) * drawn
    return jnp.clip(drawn, min=-reach, max=reach).astype(held_as)


def setup_inputs(seed: int = 0) -> dict:
    seeds = jax.random.split(jax.random.key(seed), 8)
    queries = draw_queries(jax.random.fold_in(seeds[7], 71), 0)
    keys = draw_keys(jax.random.fold_in(seeds[7], 71), 0)
    values = normal_values(seeds[2], (BATCH_SEQUENCES, SEQUENCE_LENGTH, KEY_VALUE_HEADS * HEAD_DIMENSION), 1.0, 6.0, ((0, 2), (1, 128), (2, 4)))
    output_gradient = normal_values(seeds[3], (BATCH_SEQUENCES, SEQUENCE_LENGTH, QUERY_HEADS * HEAD_DIMENSION), 1.0, 6.0, ((0, 2), (1, 128), (2, 4)))
    sinks = jnp.clip(-1.0 + 4.0 * jax.random.uniform(seeds[4], (QUERY_HEADS,), jnp.float32) ** level_of(seeds[4], (QUERY_HEADS,), ((0, 4),), -0.2, 0.2), -1.0, 3.0)
    doc_starts = draw_doc_starts(jax.random.fold_in(seeds[7], 71), 0)
    valid_counts = place_ends(jax.random.randint(seeds[6], (BATCH_SEQUENCES, N_CTX), CTX_TOK - WINDOW_LENGTH // 2, CTX_TOK + 1), jax.random.fold_in(seeds[6], 1), CTX_TOK - WINDOW_LENGTH // 2, CTX_TOK).astype(jnp.int32)
    return dict(queries=queries, keys=keys, values=values, output_gradient=output_gradient, sinks=sinks, doc_starts=doc_starts, valid_counts=valid_counts)


masked_score = -1e30


def document_ids(starts, positions):
    return jnp.sum((starts[None, :] <= positions[:, None]).astype(jnp.int32), axis=1)


def key_valid_mask(counts, positions, block_rows):
    block_index = positions // block_rows
    offset = positions - block_index * block_rows
    matches = jnp.arange(counts.shape[0], dtype=jnp.int32)[None, :] == block_index[:, None]
    limits = jnp.sum(jnp.where(matches, counts[None, :], 0), axis=1)
    return offset < limits


def band_grads(query_tile_block, key_tile_block, value_tile_block, output_grad_block, query_pos, key_pos, query_doc, key_doc, key_valid, sink_logits):
    heads_kv = key_tile_block.shape[2]
    query_group_width = query_tile_block.shape[3]
    scaling = query_tile_block.shape[4] ** -0.5
    query_wide = query_tile_block.astype(jnp.float32)
    key_wide = key_tile_block.astype(jnp.float32)
    value_wide = value_tile_block.astype(jnp.float32)
    grad_wide = output_grad_block.astype(jnp.float32)
    scores = jnp.einsum('nqhgd,nkhd->nhgqk', query_wide, key_wide) * scaling
    allowed = (key_pos[:, None, :] <= query_pos[:, :, None]) & (query_pos[:, :, None] - key_pos[:, None, :] < WINDOW_LENGTH)
    allowed = allowed & (query_doc[:, :, None] == key_doc[:, None, :]) & key_valid[:, None, :]
    scores = jnp.where(allowed[:, None, None], scores, masked_score)
    sink_term = sink_logits.reshape(heads_kv, query_group_width)[None, :, :, None]
    maxima = jnp.maximum(jnp.max(scores, axis=-1), sink_term)
    powers = jnp.exp(scores - maxima[..., None])
    sink_exp = jnp.exp(sink_term - maxima)
    denominator = jnp.sum(powers, axis=-1) + sink_exp
    attend = powers / denominator[..., None]
    attend_low = lax.optimization_barrier(attend.astype(jnp.bfloat16)).astype(jnp.float32)
    context = jnp.einsum('nhgqk,nkhd->nhgqd', attend_low, value_wide)
    deltas = jnp.sum(jnp.transpose(grad_wide, (0, 2, 3, 1, 4)) * context, axis=-1)
    grad_attend = jnp.einsum('nqhgd,nkhd->nhgqk', grad_wide, value_wide)
    grad_score = attend * (grad_attend - deltas[..., None])
    score_low = lax.optimization_barrier(grad_score.astype(jnp.bfloat16)).astype(jnp.float32)
    query_grad = jnp.einsum('nhgqk,nkhd->nqhgd', score_low, key_wide) * scaling
    key_grad = jnp.einsum('nhgqk,nqhgd->nkhd', score_low, query_wide) * scaling
    value_grad = jnp.einsum('nhgqk,nqhgd->nkhd', attend_low, grad_wide)
    sink_grad = -jnp.sum(sink_exp / denominator * deltas, axis=-1)
    return query_grad, key_grad, value_grad, sink_grad.reshape(sink_grad.shape[0], heads_kv * query_group_width)


def paired_block_tiles(sequence_rows, block_tiles, heads_kv):
    padded = jnp.concatenate([jnp.zeros((WINDOW_LENGTH, heads_kv * HEAD_DIMENSION), sequence_rows.dtype), sequence_rows], axis=0)
    padded = padded.reshape(block_tiles + 1, WINDOW_LENGTH, heads_kv, HEAD_DIMENSION)
    return jnp.concatenate([padded[:-1], padded[1:]], axis=1)


def reference(queries, keys, values, output_gradient, sinks, doc_starts, valid_counts):
    block_tiles = SEQUENCE_LENGTH // WINDOW_LENGTH
    query_group_width = QUERY_HEADS // KEY_VALUE_HEADS
    query_lines = jnp.arange(SEQUENCE_LENGTH, dtype=jnp.int32).reshape(block_tiles, WINDOW_LENGTH)
    key_lines = jnp.arange(-WINDOW_LENGTH, SEQUENCE_LENGTH, dtype=jnp.int32).reshape(block_tiles + 1, WINDOW_LENGTH)
    key_lines = jnp.concatenate([key_lines[:-1], key_lines[1:]], axis=1)
    query_list = []
    key_block_items = []
    value_block_items = []
    sink_total = jnp.zeros((QUERY_HEADS,), jnp.float32)
    for sequence_index in range(BATCH_SEQUENCES):
        query_doc = document_ids(doc_starts[sequence_index], query_lines.reshape(-1)).reshape(block_tiles, WINDOW_LENGTH)
        key_doc = document_ids(doc_starts[sequence_index], key_lines.reshape(-1)).reshape(block_tiles, 2 * WINDOW_LENGTH)
        key_valid = key_valid_mask(valid_counts[sequence_index], key_lines.reshape(-1), CTX_TOK).reshape(block_tiles, 2 * WINDOW_LENGTH)
        query_tile_block = queries[sequence_index].reshape(block_tiles, WINDOW_LENGTH, KEY_VALUE_HEADS, query_group_width, HEAD_DIMENSION)
        output_grad_block = output_gradient[sequence_index].reshape(block_tiles, WINDOW_LENGTH, KEY_VALUE_HEADS, query_group_width, HEAD_DIMENSION)
        key_tile_block = paired_block_tiles(keys[sequence_index], block_tiles, KEY_VALUE_HEADS)
        value_tile_block = paired_block_tiles(values[sequence_index], block_tiles, KEY_VALUE_HEADS)

        def per_block(entries):
            results = band_grads(*[member[None] for member in entries], sinks)
            return tuple(member[0] for member in results)

        dq_all, dk_all, dv_all, sink_part = lax.map(per_block, (query_tile_block, key_tile_block, value_tile_block, output_grad_block, query_lines, key_lines, query_doc, key_doc, key_valid))
        key_grad_overall = dk_all[:, WINDOW_LENGTH:] + jnp.concatenate([dk_all[1:, :WINDOW_LENGTH], jnp.zeros_like(dk_all[:1, :WINDOW_LENGTH])], axis=0)
        value_grad_overall = dv_all[:, WINDOW_LENGTH:] + jnp.concatenate([dv_all[1:, :WINDOW_LENGTH], jnp.zeros_like(dv_all[:1, :WINDOW_LENGTH])], axis=0)
        query_list.append(dq_all.reshape(SEQUENCE_LENGTH, QUERY_HEADS * HEAD_DIMENSION).astype(jnp.bfloat16))
        key_block_items.append(key_grad_overall.reshape(SEQUENCE_LENGTH, KEY_VALUE_HEADS * HEAD_DIMENSION).astype(jnp.bfloat16))
        value_block_items.append(value_grad_overall.reshape(SEQUENCE_LENGTH, KEY_VALUE_HEADS * HEAD_DIMENSION).astype(jnp.bfloat16))
        sink_total = sink_total + jnp.sum(sink_part, axis=0)
    return (jnp.stack(query_list), jnp.stack(key_block_items), jnp.stack(value_block_items), sink_total)
```

```python
import functools

import jax
import jax.numpy as jnp
from jax import lax
from jax.experimental import pallas as pl
from jax.experimental.pallas import tpu as pltpu
from jax.sharding import PartitionSpec as P

MESH = pl.DeviceIdType.MESH
BF16 = jnp.bfloat16
F32 = jnp.float32
T = 128
D = 64
LANES = 128
LOG2E = 1.4426950408889634
MASKED = -1e30
NX = 4


def nt(a, b):
    return lax.dot_general(a, b, (((1,), (1,)), ((), ())), preferred_element_type=F32)


def nn(a, b):
    return jnp.dot(a, b, preferred_element_type=F32)


def swap_halves(x):
    return jnp.concatenate([x[:, D:], x[:, :D]], axis=1)


def kernel(
    nz,
    ndp,
    n_seq,
    n_head,
    q_hbm,
    k_hbm,
    v_hbm,
    g_hbm,
    sinks_hbm,
    starts_hbm,
    counts_hbm,
    dq_out,
    dk_out,
    dv_out,
    sink_out,
    q,
    g,
    kv_own,
    kv_prev,
    sinks,
    starts,
    counts,
    qs,
    gs,
    kt,
    bias,
    s_own,
    p_own,
    e_buf,
    p_buf,
    stats,
    sink_acc,
    plane,
    ring,
    dkv_own,
    dkv_send,
    dkv_recv,
    dq_v,
    dkv_v,
    in_sem,
    out_sem,
    halo_send,
    halo_recv,
    grad_send,
    grad_recv,
    plane_send,
    plane_recv,
    ring_send,
    ring_recv,
):
    n_ctx = nz * NX
    ctx = lax.axis_index("ctx")
    dp = lax.axis_index("dp")
    z = ctx // NX
    x = ctx % NX
    right = (ctx + 1) % n_ctx
    left = (ctx + n_ctx - 1) % n_ctx
    n_plane = NX * ndp
    my_plane = dp * NX + x

    def plane_peer(k):
        other = (my_plane + k) % n_plane
        return {"ctx": z * NX + other % NX, "dp": other // NX}

    def ring_peer(k):
        return {"ctx": ((z + k) % nz) * NX + x}

    barrier = pltpu.get_barrier_semaphore()
    pl.semaphore_signal(barrier, inc=1, device_id={"ctx": left}, device_id_type=MESH)
    pl.semaphore_signal(barrier, inc=1, device_id={"ctx": right}, device_id_type=MESH)
    for k in range(1, n_plane):
        pl.semaphore_signal(barrier, inc=1, device_id=plane_peer(k), device_id_type=MESH)
    for k in range(1, nz):
        pl.semaphore_signal(barrier, inc=1, device_id=ring_peer(k), device_id_type=MESH)

    loads = [
        pltpu.make_async_copy(k_hbm, kv_own.at[0], in_sem.at[0]),
        pltpu.make_async_copy(v_hbm, kv_own.at[1], in_sem.at[1]),
        pltpu.make_async_copy(starts_hbm, starts, in_sem.at[2]),
        pltpu.make_async_copy(counts_hbm, counts, in_sem.at[3]),
        pltpu.make_async_copy(sinks_hbm, sinks, in_sem.at[4]),
        pltpu.make_async_copy(q_hbm, q, in_sem.at[5]),
        pltpu.make_async_copy(g_hbm, g, in_sem.at[6]),
    ]
    for copy in loads:
        copy.start()
    loads[0].wait()
    loads[1].wait()
    pl.semaphore_wait(barrier, 2 + (n_plane - 1) + (nz - 1))

    halos = []
    for b in range(n_seq):
        for t in range(2):
            copy = pltpu.make_async_remote_copy(
                src_ref=kv_own.at[t, b],
                dst_ref=kv_prev.at[t, b],
                send_sem=halo_send.at[2 * b + t],
                recv_sem=halo_recv.at[2 * b + t],
                device_id={"ctx": right},
                device_id_type=MESH,
            )
            copy.start()
            halos.append(copy)

    key_row = lax.broadcasted_iota(jnp.int32, (T, T), 0)
    query_col = lax.broadcasted_iota(jnp.int32, (T, T), 1)
    own_slot = key_row <= query_col
    lane = lax.broadcasted_iota(jnp.int32, (8, T), 1)
    pos_own = ctx * T + lane
    pos_prev = pos_own - T
    loads[2].wait()
    loads[3].wait()
    loads[4].wait()
    for b in range(n_seq):
        id_own = jnp.zeros((8, T), jnp.int32)
        id_prev = jnp.zeros((8, T), jnp.int32)
        for i in range(starts.shape[1]):
            start = starts[b, i]
            id_own += jnp.where(pos_own >= start, 1, 0)
            id_prev += jnp.where(pos_prev >= start, 1, 0)
        own_f = jnp.broadcast_to(id_own.astype(F32)[0:1], (T, T))
        prev_f = jnp.broadcast_to(id_prev.astype(F32)[0:1], (T, T))
        key_f = jnp.where(own_slot, own_f.T, prev_f.T)
        limit = jnp.where(own_slot, counts[b, ctx], jnp.where(ctx > 0, counts[b, left], 0))
        bias[b] = jnp.where((key_f == own_f) & (key_row < limit), 0.0, MASKED)

    loads[5].wait()
    loads[6].wait()
    low = lax.broadcasted_iota(jnp.int32, (T, LANES), 1) < D
    heads_per_kv = n_head // 2
    for b in range(n_seq):
        for src, dst in ((q, qs), (g, gs)):
            for pair in range(n_head // 2):
                block = src[b, :, pair * LANES : (pair + 1) * LANES]
                swapped = swap_halves(block)
                first_kv = 2 * pair < heads_per_kv
                even, odd = (block, swapped) if first_kv else (swapped, block)
                keep = low if first_kv else jnp.logical_not(low)
                zero = jnp.zeros_like(block)
                dst[b, (2 * pair) * T : (2 * pair + 1) * T, :] = jnp.where(keep, even, zero)
                dst[b, (2 * pair + 1) * T : (2 * pair + 2) * T, :] = jnp.where(keep, odd, zero)

    W = 2 * T
    n_chunk = n_head * T // W
    for b in range(n_seq):
        for c in range(n_chunk):
            cols = slice(c * W, (c + 1) * W)
            s_own[b, :, cols] = nt(kv_own[0, b], qs[b, cols, :])
            p_own[b, :, cols] = nt(kv_own[1, b], gs[b, cols, :])

    scale = D**-0.5
    own2 = lax.broadcasted_iota(jnp.int32, (T, W), 0) <= (
        lax.broadcasted_iota(jnp.int32, (T, W), 1) % T
    )
    for b in range(n_seq):
        halos[2 * b].wait_recv()
        halos[2 * b + 1].wait_recv()
        for c in range(n_chunk):
            cols = slice(c * W, (c + 1) * W)
            s_prev = nt(kv_prev[0, b], qs[b, cols, :])
            p_prev = nt(kv_prev[1, b], gs[b, cols, :])
            s = jnp.where(own2, s_own[b, :, cols], s_prev) * scale
            s = s + jnp.concatenate([bias[b], bias[b]], axis=1)
            dprob = jnp.where(own2, p_own[b, :, cols], p_prev)
            sink = jnp.concatenate(
                [jnp.full((1, T), sinks[2 * c], F32), jnp.full((1, T), sinks[2 * c + 1], F32)],
                axis=1,
            )
            top = jnp.maximum(jnp.max(s, axis=0, keepdims=True), sink)
            e = jnp.exp(s - top)
            sink_e = jnp.exp(sink - top)
            den = jnp.sum(e, axis=0, keepdims=True) + sink_e
            inv = 1.0 / den
            delta = jnp.sum(e * dprob, axis=0, keepdims=True) * inv
            e_buf[b, :, cols] = e
            p_buf[b, :, cols] = dprob
            stats[b, 0:1, cols] = inv
            stats[b, 1:2, cols] = delta
            part = sink_e * inv * delta
            for i in range(2):
                row = part[:, i * T : (i + 1) * T]
                h = 2 * c + i
                if b == 0:
                    sink_acc[h : h + 1, :] = row
                else:
                    sink_acc[h : h + 1, :] = sink_acc[h : h + 1, :] + row

    per_head = jnp.sum(sink_acc[...], axis=1, keepdims=True)
    pick = lax.broadcasted_iota(jnp.int32, (n_head, LANES), 0) == lax.broadcasted_iota(
        jnp.int32, (n_head, LANES), 1
    )
    row = jnp.sum(jnp.where(pick, per_head, 0.0), axis=0, keepdims=True)
    plane[pl.ds(my_plane, 1), :] = row

    plane_copies = []
    for k in range(1, n_plane):
        copy = pltpu.make_async_remote_copy(
            src_ref=plane.at[pl.ds(my_plane, 1)],
            dst_ref=plane.at[pl.ds(my_plane, 1)],
            send_sem=plane_send.at[k],
            recv_sem=plane_recv.at[k],
            device_id=plane_peer(k),
            device_id_type=MESH,
        )
        copy.start()
        plane_copies.append(copy)

    ring_copies = []
    grad_copies = []
    out_copies = []

    def backward(b):
        k_all = jnp.concatenate([kv_own[0, b], kv_prev[0, b]], axis=0)
        kt[...] = k_all.T
        dk = jnp.zeros((2 * T, LANES), F32)
        dv = jnp.zeros((2 * T, LANES), F32)
        for c in range(n_chunk):
            cols = slice(c * W, (c + 1) * W)
            p = e_buf[b, :, cols] * stats[b, 0:1, cols]
            ds = p * (p_buf[b, :, cols] - stats[b, 1:2, cols])
            zero = jnp.zeros_like(p)
            p_low = jnp.concatenate(
                [jnp.where(own2, p, zero).astype(BF16), jnp.where(own2, zero, p).astype(BF16)],
                axis=0,
            )
            ds_low = jnp.concatenate(
                [jnp.where(own2, ds, zero).astype(BF16), jnp.where(own2, zero, ds).astype(BF16)],
                axis=0,
            )
            dv += nn(p_low, gs[b, cols, :])
            dk += nn(ds_low, qs[b, cols, :])
            dqt = nn(kt[...], ds_low)
            kv = 0 if 2 * c < heads_per_kv else 1
            part = dqt[kv * D : (kv + 1) * D, :]
            pair = jnp.concatenate([part[:, :T], part[:, T:]], axis=0)
            dq_v[b, :, c * LANES : (c + 1) * LANES] = (pair.T * scale).astype(BF16)
        dk = dk * scale
        dkv_own[0, b] = dk[:T]
        dkv_own[1, b] = dv[:T]
        dkv_send[0, b] = dk[T:].astype(BF16)
        dkv_send[1, b] = dv[T:].astype(BF16)
        copy = pltpu.make_async_copy(dq_v.at[b], dq_out.at[b], out_sem.at[b])
        copy.start()
        out_copies.append(copy)

    backward(0)
    for copy in plane_copies:
        copy.wait_recv()
    ring[pl.ds(z, 1), :] = jnp.sum(plane[...], axis=0, keepdims=True)
    order = sorted(range(1, nz), key=lambda k: -min(k, nz - k))
    for k in order:
        copy = pltpu.make_async_remote_copy(
            src_ref=ring.at[pl.ds(z, 1)],
            dst_ref=ring.at[pl.ds(z, 1)],
            send_sem=ring_send.at[k],
            recv_sem=ring_recv.at[k],
            device_id=ring_peer(k),
            device_id_type=MESH,
        )
        copy.start()
        ring_copies.append(copy)
    for b in range(1, n_seq):
        backward(b)
    for t in range(2):
        copy = pltpu.make_async_remote_copy(
            src_ref=dkv_send.at[t],
            dst_ref=dkv_recv.at[t],
            send_sem=grad_send.at[t],
            recv_sem=grad_recv.at[t],
            device_id={"ctx": left},
            device_id_type=MESH,
        )
        copy.start()
        grad_copies.append(copy)
    not_last = jnp.where(ctx < n_ctx - 1, 1.0, 0.0)
    for t, out in ((0, dk_out), (1, dv_out)):
        grad_copies[t].wait_recv()
        dkv_v[t] = (dkv_own[t] + dkv_recv[t].astype(F32) * not_last).astype(BF16)
        copy = pltpu.make_async_copy(dkv_v.at[t], out, out_sem.at[n_seq + t])
        copy.start()
        out_copies.append(copy)
    for copy in halos + plane_copies + ring_copies + grad_copies:
        copy.wait_send()
    for copy in out_copies:
        copy.wait()
    for copy in ring_copies:
        copy.wait_recv()
    sink_out[...] = -jnp.sum(ring[...], axis=0, keepdims=True)[:, :n_head]


def solution(mesh):
    n_ctx, ndp, ntp = mesh.shape["ctx"], mesh.shape["dp"], mesh.shape["tp"]
    nz = n_ctx // NX

    def local(queries, keys, values, output_gradient, sinks, doc_starts, valid_counts):
        n_seq, rows, q_width = queries.shape
        n_head = sinks.shape[0]
        kv_width = keys.shape[2]
        any_space = pl.BlockSpec(memory_space=pl.ANY)
        cols = n_head * T
        outs = pl.pallas_call(
            functools.partial(kernel, nz, ndp, n_seq, n_head),
            out_shape=(
                jax.ShapeDtypeStruct(queries.shape, BF16),
                jax.ShapeDtypeStruct(keys.shape, BF16),
                jax.ShapeDtypeStruct(values.shape, BF16),
                jax.ShapeDtypeStruct((1, n_head), F32),
            ),
            in_specs=[any_space] * 7,
            out_specs=(
                any_space,
                any_space,
                any_space,
                pl.BlockSpec(memory_space=pltpu.VMEM),
            ),
            scratch_shapes=[
                pltpu.VMEM((n_seq, rows, q_width), BF16),
                pltpu.VMEM((n_seq, rows, q_width), BF16),
                pltpu.VMEM((2, n_seq, rows, kv_width), BF16),
                pltpu.VMEM((2, n_seq, rows, kv_width), BF16),
                pltpu.SMEM((n_head,), F32),
                pltpu.SMEM(doc_starts.shape, jnp.int32),
                pltpu.SMEM(valid_counts.shape, jnp.int32),
                pltpu.VMEM((n_seq, cols, LANES), BF16),
                pltpu.VMEM((n_seq, cols, LANES), BF16),
                pltpu.VMEM((LANES, 2 * T), BF16),
                pltpu.VMEM((n_seq, T, T), F32),
                pltpu.VMEM((n_seq, T, cols), F32),
                pltpu.VMEM((n_seq, T, cols), F32),
                pltpu.VMEM((n_seq, T, cols), F32),
                pltpu.VMEM((n_seq, T, cols), F32),
                pltpu.VMEM((n_seq, 8, cols), F32),
                pltpu.VMEM((n_head, T), F32),
                pltpu.VMEM((NX * ndp, LANES), F32),
                pltpu.VMEM((nz, LANES), F32),
                pltpu.VMEM((2, n_seq, rows, kv_width), F32),
                pltpu.VMEM((2, n_seq, rows, kv_width), BF16),
                pltpu.VMEM((2, n_seq, rows, kv_width), BF16),
                pltpu.VMEM((n_seq, rows, q_width), BF16),
                pltpu.VMEM((2, n_seq, rows, kv_width), BF16),
                pltpu.SemaphoreType.DMA((7,)),
                pltpu.SemaphoreType.DMA((n_seq + 2,)),
                pltpu.SemaphoreType.DMA((2 * n_seq,)),
                pltpu.SemaphoreType.DMA((2 * n_seq,)),
                pltpu.SemaphoreType.DMA((2,)),
                pltpu.SemaphoreType.DMA((2,)),
                pltpu.SemaphoreType.DMA((NX * ndp,)),
                pltpu.SemaphoreType.DMA((NX * ndp,)),
                pltpu.SemaphoreType.DMA((nz,)),
                pltpu.SemaphoreType.DMA((nz,)),
            ],
            compiler_params=pltpu.CompilerParams(
                collective_id=0,
                has_side_effects=True,
                vmem_limit_bytes=48 * 1024 * 1024,
            ),
        )(queries, keys, values, output_gradient, sinks, doc_starts, valid_counts)
        return outs[0], outs[1], outs[2], outs[3].reshape(n_head)

    split = P("dp", "ctx", "tp")
    return jax.shard_map(
        local,
        mesh=mesh,
        in_specs=(split, split, split, split, P("tp"), P("dp", None), P("dp", None)),
        out_specs=(split, split, split, P("tp")),
        check_vma=False,
    )
```

```python
import functools

import jax
import jax.numpy as jnp
from jax import lax
from jax.experimental import pallas as pl
from jax.experimental.pallas import tpu as pltpu
from jax.sharding import PartitionSpec as P

MESH = pl.DeviceIdType.MESH
BF16 = jnp.bfloat16
F32 = jnp.float32
T = 128
D = 64
LANES = 128
LOG2E = 1.4426950408889634
MASKED = -1e30
JUMP = 8
NX = 4


def nt(a, b):
    return lax.dot_general(a, b, (((1,), (1,)), ((), ())), preferred_element_type=F32)


def nn(a, b):
    return jnp.dot(a, b, preferred_element_type=F32)


def swap_halves(x):
    return jnp.concatenate([x[:, D:], x[:, :D]], axis=1)


def kernel(
    nz,
    ndp,
    n_seq,
    n_head,
    q_hbm,
    k_hbm,
    v_hbm,
    g_hbm,
    sinks_hbm,
    starts_hbm,
    counts_hbm,
    dq_out,
    dk_out,
    dv_out,
    sink_out,
    q,
    g,
    kv_own,
    kv_prev,
    sinks,
    starts,
    counts,
    qs,
    gs,
    kt,
    bias,
    s_own,
    p_own,
    e_buf,
    p_buf,
    stats,
    sink_acc,
    plane,
    ring,
    dkv_own,
    dkv_send,
    dkv_recv,
    in_sem,
    halo_send,
    halo_recv,
    grad_send,
    grad_recv,
    plane_send,
    plane_recv,
    ring_send,
    ring_recv,
    know_1,
    know_2,
    know_4,
):
    n_ctx = nz * NX
    ctx = lax.axis_index("ctx")
    dp = lax.axis_index("dp")
    z = ctx // NX
    x = ctx % NX
    right = (ctx + 1) % n_ctx
    left = (ctx + n_ctx - 1) % n_ctx
    n_plane = NX * ndp
    my_plane = dp * NX + x

    def plane_peer(k):
        other = (my_plane + k) % n_plane
        return {"ctx": z * NX + other % NX, "dp": other // NX}

    def ring_peer(k):
        return {"ctx": ((z + k + nz) % nz) * NX + x}

    def x_peer(k):
        return {"ctx": z * NX + (x + k) % NX}

    def greet(sem, peers):
        for peer in peers:
            pl.semaphore_signal(sem, inc=1, device_id=peer, device_id_type=MESH)

    loads = [
        pltpu.make_async_copy(k_hbm, kv_own.at[0], in_sem.at[0]),
        pltpu.make_async_copy(v_hbm, kv_own.at[1], in_sem.at[1]),
        pltpu.make_async_copy(starts_hbm, starts, in_sem.at[2]),
        pltpu.make_async_copy(counts_hbm, counts, in_sem.at[3]),
        pltpu.make_async_copy(sinks_hbm, sinks, in_sem.at[4]),
        pltpu.make_async_copy(q_hbm, q, in_sem.at[5]),
        pltpu.make_async_copy(g_hbm, g, in_sem.at[6]),
    ]
    loads[0].start()
    loads[1].start()
    barrier = pltpu.get_barrier_semaphore()
    near = [x_peer(1), x_peer(NX - 1), ring_peer(1), ring_peer(-1)]
    near += [{"dp": (dp + k) % ndp} for k in range(1, ndp)]
    greet(barrier, [{"ctx": right}, {"ctx": left}] + near)
    for copy in loads[2:]:
        copy.start()
    loads[0].wait()
    loads[1].wait()
    pl.semaphore_wait(barrier, 2 + len(near))

    halos = []
    for b in range(n_seq):
        for t in range(2):
            copy = pltpu.make_async_remote_copy(
                src_ref=kv_own.at[t, b],
                dst_ref=kv_prev.at[t, b],
                send_sem=halo_send.at[2 * b + t],
                recv_sem=halo_recv.at[2 * b + t],
                device_id={"ctx": right},
                device_id_type=MESH,
            )
            copy.start()
            halos.append(copy)
    greet(know_1, near)

    key_row = lax.broadcasted_iota(jnp.int32, (T, T), 0)
    query_col = lax.broadcasted_iota(jnp.int32, (T, T), 1)
    own_slot = key_row <= query_col
    lane = lax.broadcasted_iota(jnp.int32, (8, T), 1)
    pos_own = ctx * T + lane
    pos_prev = pos_own - T
    loads[2].wait()
    loads[3].wait()
    loads[4].wait()
    for b in range(n_seq):
        id_own = jnp.zeros((8, T), jnp.int32)
        id_prev = jnp.zeros((8, T), jnp.int32)
        for i in range(starts.shape[1]):
            start = starts[b, i]
            id_own += jnp.where(pos_own >= start, 1, 0)
            id_prev += jnp.where(pos_prev >= start, 1, 0)
        own_f = jnp.broadcast_to(id_own.astype(F32)[0:1], (T, T))
        prev_f = jnp.broadcast_to(id_prev.astype(F32)[0:1], (T, T))
        key_f = jnp.where(own_slot, own_f.T, prev_f.T)
        limit = jnp.where(own_slot, counts[b, ctx], jnp.where(ctx > 0, counts[b, left], 0))
        bias[b] = jnp.where((key_f == own_f) & (key_row < limit), 0.0, MASKED)

    loads[5].wait()
    loads[6].wait()
    low = lax.broadcasted_iota(jnp.int32, (T, LANES), 1) < D
    heads_per_kv = n_head // 2
    for b in range(n_seq):
        for src, dst in ((q, qs), (g, gs)):
            for pair in range(n_head // 2):
                block = src[b, :, pair * LANES : (pair + 1) * LANES]
                swapped = swap_halves(block)
                first_kv = 2 * pair < heads_per_kv
                even, odd = (block, swapped) if first_kv else (swapped, block)
                keep = low if first_kv else jnp.logical_not(low)
                zero = jnp.zeros_like(block)
                dst[b, (2 * pair) * T : (2 * pair + 1) * T, :] = jnp.where(keep, even, zero)
                dst[b, (2 * pair + 1) * T : (2 * pair + 2) * T, :] = jnp.where(keep, odd, zero)

    W = 2 * T
    n_chunk = n_head * T // W
    for b in range(n_seq):
        for c in range(n_chunk):
            cols = slice(c * W, (c + 1) * W)
            s_own[b, :, cols] = nt(kv_own[0, b], qs[b, cols, :])
            p_own[b, :, cols] = nt(kv_own[1, b], gs[b, cols, :])

    pl.semaphore_wait(know_1, len(near))
    next_2 = [x_peer(2), ring_peer(2), ring_peer(-2)]
    greet(know_2, next_2)

    scale = D**-0.5
    own2 = lax.broadcasted_iota(jnp.int32, (T, W), 0) <= (
        lax.broadcasted_iota(jnp.int32, (T, W), 1) % T
    )
    for b in range(n_seq):
        if b == 1:
            pl.semaphore_wait(know_2, len(next_2))
            next_4 = [ring_peer(4), ring_peer(-4)]
            greet(know_4, next_4)
        halos[2 * b].wait_recv()
        halos[2 * b + 1].wait_recv()
        for c in range(n_chunk):
            cols = slice(c * W, (c + 1) * W)
            s_prev = nt(kv_prev[0, b], qs[b, cols, :])
            p_prev = nt(kv_prev[1, b], gs[b, cols, :])
            s = jnp.where(own2, s_own[b, :, cols], s_prev) * scale
            s = s + jnp.concatenate([bias[b], bias[b]], axis=1)
            dprob = jnp.where(own2, p_own[b, :, cols], p_prev)
            sink = jnp.concatenate(
                [jnp.full((1, T), sinks[2 * c], F32), jnp.full((1, T), sinks[2 * c + 1], F32)],
                axis=1,
            )
            top = jnp.maximum(jnp.max(s, axis=0, keepdims=True), sink)
            e = jnp.exp(s - top)
            sink_e = jnp.exp(sink - top)
            den = jnp.sum(e, axis=0, keepdims=True) + sink_e
            inv = 1.0 / den
            delta = jnp.sum(e * dprob, axis=0, keepdims=True) * inv
            e_buf[b, :, cols] = e
            p_buf[b, :, cols] = dprob
            stats[b, 0:1, cols] = inv
            stats[b, 1:2, cols] = delta
            part = sink_e * inv * delta
            for i in range(2):
                row = part[:, i * T : (i + 1) * T]
                h = 2 * c + i
                if b == 0:
                    sink_acc[h : h + 1, :] = row
                else:
                    sink_acc[h : h + 1, :] = sink_acc[h : h + 1, :] + row

    per_head = jnp.sum(sink_acc[...], axis=1, keepdims=True)
    pick = lax.broadcasted_iota(jnp.int32, (n_head, LANES), 0) == lax.broadcasted_iota(
        jnp.int32, (n_head, LANES), 1
    )
    row = jnp.sum(jnp.where(pick, per_head, 0.0), axis=0, keepdims=True)
    plane[pl.ds(my_plane, 1), :] = row

    plane_copies = []
    for k in range(1, n_plane):
        copy = pltpu.make_async_remote_copy(
            src_ref=plane.at[pl.ds(my_plane, 1)],
            dst_ref=plane.at[pl.ds(my_plane, 1)],
            send_sem=plane_send.at[k],
            recv_sem=plane_recv.at[k],
            device_id=plane_peer(k),
            device_id_type=MESH,
        )
        copy.start()
        plane_copies.append(copy)

    grad_copies = []

    def backward(b):
        k_all = jnp.concatenate([kv_own[0, b], kv_prev[0, b]], axis=0)
        kt[...] = k_all.T
        dk = jnp.zeros((2 * T, LANES), F32)
        dv = jnp.zeros((2 * T, LANES), F32)
        for c in range(n_chunk):
            cols = slice(c * W, (c + 1) * W)
            p = e_buf[b, :, cols] * stats[b, 0:1, cols]
            ds = p * (p_buf[b, :, cols] - stats[b, 1:2, cols])
            zero = jnp.zeros_like(p)
            p_low = jnp.concatenate(
                [jnp.where(own2, p, zero).astype(BF16), jnp.where(own2, zero, p).astype(BF16)],
                axis=0,
            )
            ds_low = jnp.concatenate(
                [jnp.where(own2, ds, zero).astype(BF16), jnp.where(own2, zero, ds).astype(BF16)],
                axis=0,
            )
            dv += nn(p_low, gs[b, cols, :])
            dk += nn(ds_low, qs[b, cols, :])
            dqt = nn(kt[...], ds_low)
            kv = 0 if 2 * c < heads_per_kv else 1
            part = dqt[kv * D : (kv + 1) * D, :]
            pair = jnp.concatenate([part[:, :T], part[:, T:]], axis=0)
            dq_out[b, :, c * LANES : (c + 1) * LANES] = (pair.T * scale).astype(BF16)
        dk = dk * scale
        dkv_own[0, b] = dk[:T]
        dkv_own[1, b] = dv[:T]
        dkv_send[0, b] = dk[T:].astype(BF16)
        dkv_send[1, b] = dv[T:].astype(BF16)

    for b in range(n_seq):
        backward(b)
    for copy in plane_copies:
        copy.wait_recv()
    ring[pl.ds(z, 1), :] = jnp.sum(plane[...], axis=0, keepdims=True)
    pl.semaphore_wait(know_4, len(next_4))

    def send_row(k, to, sems):
        at = pl.ds((z + k + nz) % nz, 1)
        copy = pltpu.make_async_remote_copy(
            src_ref=ring.at[at],
            dst_ref=ring.at[at],
            send_sem=sems[0],
            recv_sem=sems[1],
            device_id=ring_peer(to),
            device_id_type=MESH,
        )
        copy.start()
        return copy

    up, down, far_up, far_down = {}, {}, {}, {}
    for k in range(JUMP, 0, -1):
        up[k] = send_row(0, k, (ring_send.at[k], ring_recv.at[k]))
        down[k] = send_row(0, -k, (ring_send.at[JUMP + k], ring_recv.at[JUMP + k]))
    for t in range(2):
        copy = pltpu.make_async_remote_copy(
            src_ref=dkv_send.at[t],
            dst_ref=dkv_recv.at[t],
            send_sem=grad_send.at[t],
            recv_sem=grad_recv.at[t],
            device_id={"ctx": left},
            device_id_type=MESH,
        )
        copy.start()
        grad_copies.append(copy)
    for k in range(1, JUMP + 1):
        down[k].wait_recv()
        i = 2 * JUMP + k
        far_down[k] = send_row(k, -JUMP, (ring_send.at[i], ring_recv.at[i]))
        up[k].wait_recv()
        if k < JUMP:
            i = 3 * JUMP + k
            far_up[k] = send_row(-k, JUMP, (ring_send.at[i], ring_recv.at[i]))
    far_copies = list(far_down.values()) + list(far_up.values())
    ring_copies = list(up.values()) + list(down.values()) + far_copies
    not_last = jnp.where(ctx < n_ctx - 1, 1.0, 0.0)
    for t, out in ((0, dk_out), (1, dv_out)):
        grad_copies[t].wait_recv()
        out[...] = (dkv_own[t] + dkv_recv[t].astype(F32) * not_last).astype(BF16)
    for copy in halos + plane_copies + ring_copies + grad_copies:
        copy.wait_send()
    for copy in far_copies:
        copy.wait_recv()
    sink_out[...] = -jnp.sum(ring[...], axis=0, keepdims=True)[:, :n_head]


def write_out(dq, dk, dv, sink, dq_hbm, dk_hbm, dv_hbm, sink_hbm, sem):
    pairs = ((dq, dq_hbm), (dk, dk_hbm), (dv, dv_hbm), (sink, sink_hbm))
    copies = [pltpu.make_async_copy(src, dst, sem.at[i]) for i, (src, dst) in enumerate(pairs)]
    for copy in copies:
        copy.start()
    for copy in copies:
        copy.wait()


def solution(mesh):
    n_ctx, ndp, ntp = mesh.shape["ctx"], mesh.shape["dp"], mesh.shape["tp"]
    nz = n_ctx // NX

    def local(queries, keys, values, output_gradient, sinks, doc_starts, valid_counts):
        n_seq, rows, q_width = queries.shape
        n_head = sinks.shape[0]
        kv_width = keys.shape[2]
        hbm = pl.BlockSpec(memory_space=pltpu.HBM)
        vmem = pl.BlockSpec(memory_space=pltpu.VMEM)
        cols = n_head * T
        outs = pl.pallas_call(
            functools.partial(kernel, nz, ndp, n_seq, n_head),
            out_shape=(
                pltpu.VMEM(queries.shape, BF16),
                pltpu.VMEM(keys.shape, BF16),
                pltpu.VMEM(values.shape, BF16),
                pltpu.VMEM((1, n_head), F32),
            ),
            in_specs=[hbm] * 7,
            out_specs=(vmem,) * 4,
            scratch_shapes=[
                pltpu.VMEM((n_seq, rows, q_width), BF16),
                pltpu.VMEM((n_seq, rows, q_width), BF16),
                pltpu.VMEM((2, n_seq, rows, kv_width), BF16),
                pltpu.VMEM((2, n_seq, rows, kv_width), BF16),
                pltpu.SMEM((n_head,), F32),
                pltpu.SMEM(doc_starts.shape, jnp.int32),
                pltpu.SMEM(valid_counts.shape, jnp.int32),
                pltpu.VMEM((n_seq, cols, LANES), BF16),
                pltpu.VMEM((n_seq, cols, LANES), BF16),
                pltpu.VMEM((LANES, 2 * T), BF16),
                pltpu.VMEM((n_seq, T, T), F32),
                pltpu.VMEM((n_seq, T, cols), F32),
                pltpu.VMEM((n_seq, T, cols), F32),
                pltpu.VMEM((n_seq, T, cols), F32),
                pltpu.VMEM((n_seq, T, cols), F32),
                pltpu.VMEM((n_seq, 8, cols), F32),
                pltpu.VMEM((n_head, T), F32),
                pltpu.VMEM((NX * ndp, LANES), F32),
                pltpu.VMEM((nz, LANES), F32),
                pltpu.VMEM((2, n_seq, rows, kv_width), F32),
                pltpu.VMEM((2, n_seq, rows, kv_width), BF16),
                pltpu.VMEM((2, n_seq, rows, kv_width), BF16),
                pltpu.SemaphoreType.DMA((7,)),
                pltpu.SemaphoreType.DMA((2 * n_seq,)),
                pltpu.SemaphoreType.DMA((2 * n_seq,)),
                pltpu.SemaphoreType.DMA((2,)),
                pltpu.SemaphoreType.DMA((2,)),
                pltpu.SemaphoreType.DMA((NX * ndp,)),
                pltpu.SemaphoreType.DMA((NX * ndp,)),
                pltpu.SemaphoreType.DMA((4 * JUMP + 1,)),
                pltpu.SemaphoreType.DMA((4 * JUMP + 1,)),
                pltpu.SemaphoreType.REGULAR,
                pltpu.SemaphoreType.REGULAR,
                pltpu.SemaphoreType.REGULAR,
            ],
            compiler_params=pltpu.CompilerParams(
                collective_id=0,
                has_side_effects=True,
                vmem_limit_bytes=48 * 1024 * 1024,
            ),
        )(*[pltpu.with_memory_space_constraint(a, pltpu.HBM) for a in (queries, keys, values, output_gradient, sinks, doc_starts, valid_counts)])
        outs = pl.pallas_call(
            write_out,
            out_shape=(
                jax.ShapeDtypeStruct(queries.shape, BF16),
                jax.ShapeDtypeStruct(keys.shape, BF16),
                jax.ShapeDtypeStruct(values.shape, BF16),
                jax.ShapeDtypeStruct((1, n_head), F32),
            ),
            in_specs=[vmem] * 4,
            out_specs=(hbm,) * 4,
            scratch_shapes=[pltpu.SemaphoreType.DMA((4,))],
            compiler_params=pltpu.CompilerParams(vmem_limit_bytes=1024 * 1024),
        )(*outs)
        return outs[0], outs[1], outs[2], outs[3].reshape(n_head)

    split = P("dp", "ctx", "tp")
    return jax.shard_map(
        local,
        mesh=mesh,
        in_specs=(split, split, split, split, P("tp"), P("dp", None), P("dp", None)),
        out_specs=(split, split, split, P("tp")),
        check_vma=False,
    )
```
